32 devices in a mesh: groups: 2 (over x), expert: 16 (over z, y, core).
Axes of the slice: x: 2, y: 2, z: 4, core: 2. Of those that a mesh axis runs over, the one named last changes fastest.
Arguments:
- tokens: bfloat16 [256, 6144], P(('groups', 'expert')), parts along dimension 0, may hold values from -6 to 6
- norm_gain: float32 [6144], replicated, may hold values from 0.5 to 1.5
- router: bfloat16 [6144, 4], replicated, may hold values from -0.078125 to 0.078125
- w_gate: bfloat16 [6144, 4096], P(None, 'expert'), may hold values from -0.078125 to 0.078125
- w_up: bfloat16 [6144, 4096], P(None, 'expert'), may hold values from -0.078125 to 0.078125
- w_down: bfloat16 [4096, 6144], P('expert'), may hold values from -0.1875 to 0.1875
- expert_ids: int32 [256, 2], P(('groups', 'expert')), parts along dimension 0, may hold values from 0 to 3, as said below
- live_rows: int32 [32], P(('groups', 'expert')), parts along dimension 0, may hold values from 6 to 8, as said below
Outputs:
- mixed_out: bfloat16 [256, 6144], P(('groups', 'expert')), parts along dimension 0
The draws below stay inside these ranges and needn't reach their ends.
There are 2 independent parts, one for each index of `groups`. The reference program is written for one: setup_inputs(seed, part) draws one part's arguments, and reference() takes and returns one part's arrays. A program takes and returns all parts, laid end to end along the dimension named above; an argument that names none is the same for every part. Nothing has to cross between parts.
Inputs may be any that keep to these rules, and one draw needn't show every extreme that they name: `expert_ids`: each row names two different experts. Among the live rows of one device no expert is named by more than 6 rows; in every draw some expert is named by exactly 6 live rows of every device. `live_rows`: rows at or beyond this count in a device's block are padding; some device is full in every draw.
All inputs are finite; a program needn't handle non-finite values.
Results may differ from the reference program's by a relative error of at most 0.0042.
Values may be sent and summed in bfloat16 or wider, within the bound.
No kernel may reach another device: no remote copies, remote signals or barrier semaphores. Data moves between devices by JAX's collectives and lax.ppermute only.
A program may use at most 128 MiB of HBM per device.

```python
import jax
import jax.numpy as jnp
from jax import lax

D = 6144
EXPERTS = 4
FF_DEV = 256
B_DEV = 8
CAP = 6
FF = 1024
TOKENS = 128
N_EXPERT = 16


def routing_tables(key):
    base = jax.random.fold_in(key, 23)
    keys = jax.random.split(base, 6)
    hot = jax.random.randint(keys[0], (), 0, EXPERTS)
    live_count = jax.random.randint(keys[1], (N_EXPERT,), CAP, B_DEV + 1)
    full_device = jax.random.randint(keys[2], (), 0, N_EXPERT)
    live_count = jnp.where(jnp.arange(N_EXPERT) == full_device, B_DEV, live_count)
    shifted = jax.random.randint(keys[3], (N_EXPERT,), 0, B_DEV) % live_count
    offset = jax.random.randint(keys[4], (N_EXPERT, 1), 0, EXPERTS - 1)
    flipped = jax.random.randint(keys[5], (N_EXPERT, B_DEV), 0, 2)
    rank = (jnp.arange(B_DEV)[None, :] + shifted[:, None]) % live_count[:, None]
    spare = EXPERTS - 1
    first_other = (hot + 1 + (offset + rank) % spare) % EXPERTS
    second_other = (hot + 1 + (offset + rank + 1) % spare) % EXPERTS
    leading = jnp.where(rank < CAP, hot, first_other)
    trailing = jnp.where(rank < CAP, first_other, second_other)
    first_pick = jnp.where(flipped == 1, trailing, leading)
    second_pick = jnp.where(flipped == 1, leading, trailing)
    chosen_ids = jnp.stack([first_pick, second_pick], axis=-1).reshape(N_EXPERT * B_DEV, 2)
    return (chosen_ids.astype(jnp.int32), live_count.astype(jnp.int32))


def draw_expert_ids(key, part):
    return routing_tables(key)[0]


def draw_live_rows(key, part):
    return routing_tables(key)[1]


def level_of(stream_key, dims, shards, smallest, largest):
    factor_of = 1.0
    for axis_at, parts in shards:
        steps = jax.random.uniform(jax.random.fold_in(jax.random.fold_in(stream_key, 6), axis_at), (parts,), jnp.float32, smallest / len(shards), largest / len(shards))
        factor_of = factor_of * jnp.repeat(jnp.exp(steps), dims[axis_at] // parts).reshape((-1,) + (1,) * (len(dims) - 1 - axis_at))
    return factor_of


def scatter_about(stream_key, dims, width, limit, cuts=(), kind=jnp.bfloat16):
    loudness = level_of(stream_key, dims, cuts, -0.22, 0.18) if cuts else 1.0
    result = jax.random.normal(stream_key, dims, jnp.float32) * width * loudness
    return jnp.minimum(jnp.maximum(result, -limit), limit).astype(kind)


def setup_inputs(seed: int = 0, part: int = 0) -> dict:
    seeds = jax.random.split(jax.random.key(seed), 9)
    part_splits = jax.random.split(jax.random.fold_in(seeds[8], part), 9)
    return {
        "tokens": scatter_about(part_splits[0], (TOKENS, D), 1.0, 6.0, ((0, 16),)),
        "norm_gain": jnp.clip(1.0 + 0.1 * jax.random.normal(seeds[1], (D,), jnp.float32), 0.5, 1.5),
        "router": scatter_about(seeds[2], (D, EXPERTS), D ** -0.5, 0.078125),
        "w_gate": scatter_about(seeds[3], (D, EXPERTS * FF), D ** -0.5, 0.078125, ((1, 16),)),
        "w_up": scatter_about(seeds[4], (D, EXPERTS * FF), D ** -0.5, 0.078125, ((1, 16),)),
        "w_down": scatter_about(seeds[5], (EXPERTS * FF, D), FF ** -0.5, 0.1875, ((0, 16),)),
        "expert_ids": draw_expert_ids(jax.random.fold_in(jax.random.fold_in(seeds[8], part), 71), part),
        "live_rows": draw_live_rows(jax.random.fold_in(jax.random.fold_in(seeds[8], part), 71), part),
    }


epsilon = 1e-05

def rms_normed(tokens, norm_gain):
    tok_f32 = tokens.astype(jnp.float32)
    scale_inv = lax.rsqrt(lax.optimization_barrier(jnp.mean(tok_f32 * tok_f32, axis=-1, keepdims=True)) + epsilon)
    return (tok_f32 * scale_inv * norm_gain).astype(jnp.bfloat16)

def add_block(running, block_pair):
    partial_value = jnp.dot(block_pair[0], block_pair[1], preferred_element_type=jnp.float32).astype(jnp.bfloat16)
    partial_value = lax.optimization_barrier(partial_value)
    return (running + partial_value.astype(jnp.float32), None)

def reference(tokens, norm_gain, router, w_gate, w_up, w_down, expert_ids, live_rows):
    normed = rms_normed(tokens, norm_gain)
    logits = jnp.dot(normed, router, preferred_element_type=jnp.float32)
    one_hot = (expert_ids[:, :, None] == jnp.arange(EXPERTS, dtype=jnp.int32)[None, None, :]).astype(jnp.float32)
    chosen = lax.optimization_barrier(jnp.sum(one_hot * logits[:, None, :], axis=-1))
    gate_probs = jax.nn.sigmoid(chosen - chosen[:, ::-1])
    positions = jnp.arange(TOKENS, dtype=jnp.int32)
    alive_mask = (positions % B_DEV < live_rows[positions // B_DEV]).astype(jnp.float32)
    expert_weight = lax.optimization_barrier(jnp.sum(one_hot * (gate_probs * alive_mask[:, None])[:, :, None], axis=1))
    members = FF // FF_DEV
    routed_out = jnp.zeros((TOKENS, D), jnp.float32)
    for expert in range(EXPERTS):
        gate_proj = jnp.dot(normed, w_gate[:, expert * FF:(expert + 1) * FF], preferred_element_type=jnp.float32)
        up_proj = jnp.dot(normed, w_up[:, expert * FF:(expert + 1) * FF], preferred_element_type=jnp.float32)
        hidden = (jax.nn.silu(gate_proj) * up_proj).astype(jnp.bfloat16)
        blocks_hidden = hidden.reshape(TOKENS, members, FF_DEV).transpose(1, 0, 2)
        blocks_down = w_down[expert * FF:(expert + 1) * FF].reshape(members, FF_DEV, D)
        expert_out, unused = lax.scan(add_block, jnp.zeros((TOKENS, D), jnp.float32), (blocks_hidden, blocks_down))
        routed_out = routed_out + expert_weight[:, expert:expert + 1] * expert_out
    return (tokens.astype(jnp.float32) + routed_out).astype(jnp.bfloat16)
```

```python
import functools

import jax
import jax.numpy as jnp
from jax import lax
from jax.experimental import pallas as pl
from jax.experimental.pallas import tpu as pltpu
from jax.sharding import PartitionSpec as P

CAP = 6
SUB = 8
EPS = 1e-05
CORES = 2
F32 = jnp.float32
BF16 = jnp.bfloat16


VMEM = pl.BlockSpec(memory_space=pltpu.VMEM)
SMEM = pl.BlockSpec(memory_space=pltpu.SMEM)


def dot(a, b):
    return jnp.dot(a, b, preferred_element_type=F32)


def packing(width):
    main = width * CAP // SUB
    tail = width - main
    blocks = main // tail
    return main, tail, blocks


def pre_kernel(experts, z_ref, live_ref, ids_ref, tok_ref, gain_ref, router_ref, *outs):
    pieces, table_ref = outs[:-1], outs[-1]
    rows, width = tok_ref.shape
    main, tail, blocks = packing(width)
    lanes = table_ref.shape[1]
    tok = tok_ref[...].astype(F32)
    scale = lax.rsqrt(jnp.mean(tok * tok, axis=-1, keepdims=True) + EPS)
    normed = (tok * scale * gain_ref[...]).astype(BF16)
    normed_f32 = normed.astype(F32)

    row = lax.broadcasted_iota(jnp.int32, (rows, lanes), 0)
    lane = lax.broadcasted_iota(jnp.int32, (rows, lanes), 1)
    first = jnp.zeros((rows, lanes), jnp.int32)
    second = jnp.zeros((rows, lanes), jnp.int32)
    for t in range(rows):
        first = jnp.where(row == t, ids_ref[0, t], first)
        second = jnp.where(row == t, ids_ref[1, t], second)
    alive = row < live_ref[0]
    logits = [
        jnp.sum(normed_f32 * router_ref[e : e + 1, :].astype(F32), axis=-1, keepdims=True)
        for e in range(experts)
    ]
    logit_first = jnp.zeros((rows, lanes), F32)
    logit_second = jnp.zeros((rows, lanes), F32)
    for e in range(experts):
        logit_first = jnp.where(first == e, logits[e], logit_first)
        logit_second = jnp.where(second == e, logits[e], logit_second)
    prob_first = 1.0 / (1.0 + jnp.exp(logit_second - logit_first))
    prob_second = 1.0 / (1.0 + jnp.exp(logit_first - logit_second))

    r = lane % SUB
    k = (lane // SUB) % experts
    j = lane // (SUB * experts)
    expert = k ^ z_ref[0]
    is_first = first == expert
    is_second = second == expert
    member = jnp.logical_and(jnp.logical_or(is_first, is_second), alive).astype(F32)
    slot = jnp.zeros((rows, lanes), F32)
    for t in range(rows - 1):
        slot = slot + jnp.where(row > t, member[t : t + 1, :], 0.0)
    main_slot = jnp.where(r < CAP, r, SUB)
    tail_slot = jnp.where(r < CAP, SUB, (r - CAP) * blocks + j - 1)
    wanted = jnp.where(j == 0, main_slot, tail_slot).astype(F32)
    placed = jnp.where(slot == wanted, member, 0.0)
    gate = jnp.where(is_first, prob_first, prob_second)
    table_ref[...] = placed * gate

    step = experts * SUB
    pick = placed.astype(BF16)
    for i in range(blocks):
        both = jnp.concatenate([pick[:, :step], pick[:, (1 + i) * step : (2 + i) * step]], axis=0)
        data = jnp.concatenate([normed[:, i * tail : (i + 1) * tail], normed[:, main:]], axis=0)
        block = lax.dot_general(both, data, (((0,), (0,)), ((), ())), preferred_element_type=F32).astype(BF16)
        for n, piece in enumerate(pieces):
            piece[:, i * tail : (i + 1) * tail] = block[n * SUB : (n + 1) * SUB, :]


def pre(tokens, norm_gain, router, expert_ids, live_rows, plane):
    rows, width = tokens.shape
    experts = router.shape[1]
    main, _, blocks = packing(width)
    lanes = (1 + blocks) * experts * SUB
    return pl.pallas_call(
        functools.partial(pre_kernel, experts),
        out_shape=[jax.ShapeDtypeStruct((SUB, main), BF16)] * experts + [jax.ShapeDtypeStruct((rows, lanes), F32)],
        in_specs=[SMEM, SMEM, SMEM, VMEM, VMEM, VMEM],
        out_specs=[VMEM] * (experts + 1),
        name="pre",
    )(plane.reshape(1), live_rows, expert_ids.T, tokens, norm_gain.reshape(1, width), router.T)


def ffn_kernel(count, *refs):
    pieces = refs[:count]
    wg_ref, wu_ref, wd_ref = refs[count : count + 3]
    keep_ref, give_ref, x_ref = refs[count + 3 :]
    width = wg_ref.shape[0]
    hidden_width = wg_ref.shape[1]
    main, tail, blocks = packing(width)
    at = 0
    for piece in pieces:
        n = piece.shape[0]
        x_ref[at : at + n, :] = piece[...]
        at += n
    total = at
    half = total // 2
    size = 128 if total % 128 == 0 else total
    row = lax.broadcasted_iota(jnp.int32, (size, size), 0)
    col = lax.broadcasted_iota(jnp.int32, (size, size), 1)
    same = row // SUB == col // SUB
    in_row = lax.broadcasted_iota(jnp.int32, (size, hidden_width), 0) % SUB

    def chunk(base):
        x = x_ref[pl.ds(base, size), :]
        rest = jnp.zeros((size, tail), F32)
        for i in range(blocks):
            take = jnp.logical_and(same, row % SUB == (col % SUB - CAP) * blocks + i)
            take = jnp.logical_and(take, col % SUB >= CAP)
            rest = rest + dot(take.astype(BF16), x[:, i * tail : (i + 1) * tail])
        rest = rest.astype(BF16)
        gate = dot(x, wg_ref[:main, :]) + dot(rest, wg_ref[main:, :])
        up = dot(x, wu_ref[:main, :]) + dot(rest, wu_ref[main:, :])
        hidden = (gate / (1.0 + jnp.exp(-gate)) * up).astype(BF16)
        upper = jnp.where(in_row < CAP, hidden, jnp.zeros_like(hidden))
        for i in range(blocks):
            give = jnp.logical_and(same, col % SUB == (row % SUB - CAP) * blocks + i)
            give = jnp.logical_and(give, row % SUB >= CAP)
            lower = dot(give.astype(BF16), hidden).astype(BF16)
            cols = slice(i * tail, (i + 1) * tail)
            out = (dot(upper, wd_ref[:, cols]) + dot(lower, wd_ref[:, main:])).astype(BF16)
            x_ref[pl.ds(base, size), cols] = out

    if total == size:
        chunk(0)
    else:
        lax.fori_loop(0, total // size, lambda n, c: (chunk(pl.multiple_of(n * size, size)), c)[1], 0)
    keep_ref[...] = x_ref[:half, :]
    give_ref[...] = x_ref[half:, :]


def ffn(pieces, w_gate, w_up, w_down):
    total = sum(p.shape[0] for p in pieces)
    main = pieces[0].shape[1]
    half = jax.ShapeDtypeStruct((total // 2, main), BF16)
    return pl.pallas_call(
        functools.partial(ffn_kernel, len(pieces)),
        out_shape=[half, half],
        in_specs=[VMEM] * (len(pieces) + 3),
        out_specs=[VMEM, VMEM],
        scratch_shapes=[pltpu.VMEM((total, main), BF16)],
        name="ffn",
    )(*pieces, w_gate, w_up, w_down)


def combine_kernel(experts, table_ref, tok_ref, *refs):
    pieces, out_ref = refs[:-1], refs[-1]
    width = tok_ref.shape[1]
    main, tail, blocks = packing(width)
    step = experts * SUB
    table = table_ref[...]
    high = table.astype(BF16)
    low = (table - high.astype(F32)).astype(BF16)
    rest = jnp.zeros((tok_ref.shape[0], tail), F32)
    for i in range(blocks):
        cols = slice(i * tail, (i + 1) * tail)
        data = jnp.concatenate([p[:, cols].astype(BF16) for p in pieces], axis=0)
        mine, theirs = slice(0, step), slice((1 + i) * step, (2 + i) * step)
        out_ref[:, cols] = (
            tok_ref[:, cols].astype(F32) + dot(high[:, mine], data) + dot(low[:, mine], data)
        ).astype(BF16)
        rest = rest + dot(high[:, theirs], data) + dot(low[:, theirs], data)
    out_ref[:, main:] = (tok_ref[:, main:].astype(F32) + rest).astype(BF16)


def combine(table, tokens, pieces):
    experts = len(pieces)
    return pl.pallas_call(
        functools.partial(combine_kernel, experts),
        out_shape=jax.ShapeDtypeStruct(tokens.shape, BF16),
        in_specs=[VMEM] * (2 + experts),
        out_specs=VMEM,
        name="combine",
    )(table, tokens, *pieces)


def local(tokens, norm_gain, router, w_gate, w_up, w_down, expert_ids, live_rows):
    devices = lax.axis_size("expert")
    experts = router.shape[1]
    members = devices // experts
    lines = members // CORES

    def swap(value, distance):
        return lax.ppermute(value, "expert", [(i, i ^ distance) for i in range(devices)])

    plane = lax.axis_index("expert") // members
    *outgoing, table = pre(tokens, norm_gain, router, expert_ids, live_rows, plane)

    def add(a, b):
        return (a.astype(F32) + b.astype(F32)).astype(BF16)

    arrived = [outgoing[0]] + [swap(outgoing[k], k * members) for k in range(1, experts)]
    near = list(arrived)
    for y in range(1, lines):
        near += [swap(p, y * CORES) for p in arrived]
    pieces = near + [swap(p, 1) for p in near]
    keep, give = ffn(pieces, w_gate, w_up, w_down)
    kept = add(keep, swap(give, 1)).reshape(lines, experts, SUB, -1)
    home = []
    for k in range(experts):
        total = kept[0, k]
        for y in range(1, lines):
            total = add(total, swap(kept[y, k], y * CORES))
        home.append(swap(total, k * members) if k else total)
    return combine(table, tokens, home)


def solution(mesh):
    return jax.shard_map(
        local,
        mesh=mesh,
        in_specs=(
            P(("groups", "expert"), None),
            P(),
            P(),
            P(None, "expert"),
            P(None, "expert"),
            P("expert", None),
            P(("groups", "expert"), None),
            P(("groups", "expert")),
        ),
        out_specs=P(("groups", "expert"), None),
        check_vma=False,
    )
```

```python
import functools

import jax
import jax.numpy as jnp
from jax import lax
from jax.experimental import pallas as pl
from jax.experimental.pallas import tpu as pltpu
from jax.sharding import PartitionSpec as P

CAP = 6
SUB = 8
EPS = 1e-05
CORES = 2
F32 = jnp.float32
BF16 = jnp.bfloat16


VMEM = pl.BlockSpec(memory_space=pltpu.VMEM)
SMEM = pl.BlockSpec(memory_space=pltpu.SMEM)


def near(value):
    return pltpu.with_memory_space_constraint(value, pltpu.VMEM)


def room(mebibytes):
    return pltpu.CompilerParams(vmem_limit_bytes=mebibytes << 20)


def far(value):
    return pltpu.with_memory_space_constraint(value, pltpu.HBM)


def dot(a, b):
    return jnp.dot(a, b, preferred_element_type=F32)


def packing(width):
    main = width * CAP // SUB
    tail = width - main
    blocks = main // tail
    return main, tail, blocks


def pre_kernel(experts, z_ref, live_ref, ids_ref, tok_ref, gain_ref, router_ref, *outs):
    pieces, table_ref = outs[:-1], outs[-1]
    rows, width = tok_ref.shape
    main, tail, blocks = packing(width)
    lanes = table_ref.shape[1]
    tok = tok_ref[...].astype(F32)
    scale = lax.rsqrt(jnp.mean(tok * tok, axis=-1, keepdims=True) + EPS)
    normed = (tok * scale * gain_ref[...]).astype(BF16)
    normed_f32 = normed.astype(F32)

    row = lax.broadcasted_iota(jnp.int32, (rows, lanes), 0)
    lane = lax.broadcasted_iota(jnp.int32, (rows, lanes), 1)
    first = jnp.zeros((rows, lanes), jnp.int32)
    second = jnp.zeros((rows, lanes), jnp.int32)
    for t in range(rows):
        first = jnp.where(row == t, ids_ref[0, t], first)
        second = jnp.where(row == t, ids_ref[1, t], second)
    alive = row < live_ref[0]
    logits = [
        jnp.sum(normed_f32 * router_ref[e : e + 1, :].astype(F32), axis=-1, keepdims=True)
        for e in range(experts)
    ]
    logit_first = jnp.zeros((rows, lanes), F32)
    logit_second = jnp.zeros((rows, lanes), F32)
    for e in range(experts):
        logit_first = jnp.where(first == e, logits[e], logit_first)
        logit_second = jnp.where(second == e, logits[e], logit_second)
    prob_first = 1.0 / (1.0 + jnp.exp(logit_second - logit_first))
    prob_second = 1.0 / (1.0 + jnp.exp(logit_first - logit_second))

    r = lane % SUB
    k = (lane // SUB) % experts
    j = lane // (SUB * experts)
    expert = k ^ z_ref[0]
    is_first = first == expert
    is_second = second == expert
    member = jnp.logical_and(jnp.logical_or(is_first, is_second), alive).astype(F32)
    slot = jnp.zeros((rows, lanes), F32)
    for t in range(rows - 1):
        slot = slot + jnp.where(row > t, member[t : t + 1, :], 0.0)
    main_slot = jnp.where(r < CAP, r, SUB)
    tail_slot = jnp.where(r < CAP, SUB, (r - CAP) * blocks + j - 1)
    wanted = jnp.where(j == 0, main_slot, tail_slot).astype(F32)
    placed = jnp.where(slot == wanted, member, 0.0)
    gate = jnp.where(is_first, prob_first, prob_second)
    table_ref[...] = placed * gate

    step = experts * SUB
    pick = placed.astype(BF16)
    for i in range(blocks):
        both = jnp.concatenate([pick[:, :step], pick[:, (1 + i) * step : (2 + i) * step]], axis=0)
        data = jnp.concatenate([normed[:, i * tail : (i + 1) * tail], normed[:, main:]], axis=0)
        block = lax.dot_general(both, data, (((0,), (0,)), ((), ())), preferred_element_type=F32).astype(BF16)
        for n, piece in enumerate(pieces):
            piece[:, i * tail : (i + 1) * tail] = block[n * SUB : (n + 1) * SUB, :]


def pre(tokens, norm_gain, router, expert_ids, live_rows, plane):
    rows, width = tokens.shape
    experts = router.shape[1]
    main, _, blocks = packing(width)
    lanes = (1 + blocks) * experts * SUB
    return pl.pallas_call(
        functools.partial(pre_kernel, experts),
        out_shape=[pltpu.VMEM((SUB, main), BF16)] * experts + [pltpu.VMEM((rows, lanes), F32)],
        in_specs=[SMEM, SMEM, SMEM, VMEM, VMEM, VMEM],
        out_specs=[VMEM] * (experts + 1),
        compiler_params=room(8),
        name="pre",
    )(plane.reshape(1), live_rows, far(expert_ids.T), far(tokens), far(norm_gain.reshape(1, width)), far(router.T))


def fetch_kernel(*refs):
    count = len(refs) // 3
    copies = [
        pltpu.make_async_copy(source, target, sem)
        for source, target, sem in zip(refs[:count], refs[count + 1 : 2 * count + 1], refs[2 * count + 1 :])
    ]
    for copy in copies:
        copy.start()
    for copy in copies:
        copy.wait()


def fetch(after, *weights):
    return pl.pallas_call(
        fetch_kernel,
        out_shape=[pltpu.VMEM(w.shape, w.dtype) for w in weights],
        in_specs=[pl.BlockSpec(memory_space=pltpu.HBM)] * len(weights) + [VMEM],
        out_specs=[VMEM] * len(weights),
        scratch_shapes=[pltpu.SemaphoreType.DMA(())] * len(weights),
        compiler_params=room(1),
        cost_estimate=pl.CostEstimate(flops=10**9, bytes_accessed=sum(w.size * 2 for w in weights), transcendentals=0),
        name="fetch",
    )(*map(far, weights), near(after))


def ffn_kernel(count, *refs):
    pieces = refs[:count]
    wg_ref, wu_ref, wd_ref = refs[count : count + 3]
    keep_ref, give_ref, x_ref = refs[count + 3 :]
    width = wg_ref.shape[0]
    hidden_width = wg_ref.shape[1]
    main, tail, blocks = packing(width)
    at = 0
    for piece in pieces:
        n = piece.shape[0]
        x_ref[at : at + n, :] = piece[...]
        at += n
    total = at
    half = total // 2
    size = 128 if total % 128 == 0 else total
    row = lax.broadcasted_iota(jnp.int32, (size, size), 0)
    col = lax.broadcasted_iota(jnp.int32, (size, size), 1)
    same = row // SUB == col // SUB
    in_row = lax.broadcasted_iota(jnp.int32, (size, hidden_width), 0) % SUB

    def chunk(base):
        x = x_ref[pl.ds(base, size), :]
        rest = jnp.zeros((size, tail), F32)
        for i in range(blocks):
            take = jnp.logical_and(same, row % SUB == (col % SUB - CAP) * blocks + i)
            take = jnp.logical_and(take, col % SUB >= CAP)
            rest = rest + dot(take.astype(BF16), x[:, i * tail : (i + 1) * tail])
        rest = rest.astype(BF16)
        gate = dot(x, wg_ref[:main, :]) + dot(rest, wg_ref[main:, :])
        up = dot(x, wu_ref[:main, :]) + dot(rest, wu_ref[main:, :])
        hidden = (gate / (1.0 + jnp.exp(-gate)) * up).astype(BF16)
        upper = jnp.where(in_row < CAP, hidden, jnp.zeros_like(hidden))
        for i in range(blocks):
            give = jnp.logical_and(same, col % SUB == (row % SUB - CAP) * blocks + i)
            give = jnp.logical_and(give, row % SUB >= CAP)
            lower = dot(give.astype(BF16), hidden).astype(BF16)
            cols = slice(i * tail, (i + 1) * tail)
            out = (dot(upper, wd_ref[:, cols]) + dot(lower, wd_ref[:, main:])).astype(BF16)
            x_ref[pl.ds(base, size), cols] = out

    if total == size:
        chunk(0)
    else:
        lax.fori_loop(0, total // size, lambda n, c: (chunk(pl.multiple_of(n * size, size)), c)[1], 0)
    keep_ref[...] = x_ref[:half, :]
    give_ref[...] = x_ref[half:, :]


def ffn(pieces, weights):
    total = sum(p.shape[0] for p in pieces)
    main = pieces[0].shape[1]
    half = pltpu.VMEM((total // 2, main), BF16)
    return pl.pallas_call(
        functools.partial(ffn_kernel, len(pieces)),
        out_shape=[half, half],
        in_specs=[VMEM] * (len(pieces) + 3),
        out_specs=[VMEM, VMEM],
        scratch_shapes=[pltpu.VMEM((total, main), BF16)],
        compiler_params=room(16),
        name="ffn",
    )(*map(near, pieces), *map(near, weights))


def combine_kernel(experts, table_ref, tok_ref, *refs):
    pieces, out_ref = refs[:-1], refs[-1]
    width = tok_ref.shape[1]
    main, tail, blocks = packing(width)
    step = experts * SUB
    table = table_ref[...]
    high = table.astype(BF16)
    low = (table - high.astype(F32)).astype(BF16)
    rest = jnp.zeros((tok_ref.shape[0], tail), F32)
    for i in range(blocks):
        cols = slice(i * tail, (i + 1) * tail)
        data = jnp.concatenate([p[:, cols].astype(BF16) for p in pieces], axis=0)
        mine, theirs = slice(0, step), slice((1 + i) * step, (2 + i) * step)
        out_ref[:, cols] = (
            tok_ref[:, cols].astype(F32) + dot(high[:, mine], data) + dot(low[:, mine], data)
        ).astype(BF16)
        rest = rest + dot(high[:, theirs], data) + dot(low[:, theirs], data)
    out_ref[:, main:] = (tok_ref[:, main:].astype(F32) + rest).astype(BF16)


def combine(table, tokens, pieces):
    experts = len(pieces)
    return pl.pallas_call(
        functools.partial(combine_kernel, experts),
        out_shape=jax.ShapeDtypeStruct(tokens.shape, BF16),
        in_specs=[VMEM] * (2 + experts),
        out_specs=VMEM,
        compiler_params=room(8),
        name="combine",
    )(near(table), near(tokens), *map(near, pieces))


def local(tokens, norm_gain, router, w_gate, w_up, w_down, expert_ids, live_rows):
    devices = lax.axis_size("expert")
    experts = router.shape[1]
    members = devices // experts
    lines = members // CORES

    def swap(value, distance):
        return lax.ppermute(value, "expert", [(i, i ^ distance) for i in range(devices)])

    plane = lax.axis_index("expert") // members
    *outgoing, table = pre(tokens, norm_gain, router, expert_ids, live_rows, plane)

    def add(a, b):
        return (a.astype(F32) + b.astype(F32)).astype(BF16)

    weights = fetch(table, w_gate, w_up, w_down)
    arrived = [outgoing[0]] + [swap(outgoing[k], k * members) for k in range(1, experts)]
    held = list(arrived)
    for y in range(1, lines):
        held += [swap(p, y * CORES) for p in arrived]
    pieces = held + [swap(p, 1) for p in held]
    keep, give = ffn(pieces, weights)
    kept = add(keep, swap(give, 1)).reshape(lines, experts, SUB, -1)
    home = []
    for k in range(experts):
        total = kept[0, k]
        for y in range(1, lines):
            total = add(total, swap(kept[y, k], y * CORES))
        home.append(swap(total, k * members) if k else total)
    return combine(table, tokens, home)


def solution(mesh):
    return jax.shard_map(
        local,
        mesh=mesh,
        in_specs=(
            P(("groups", "expert"), None),
            P(),
            P(),
            P(None, "expert"),
            P(None, "expert"),
            P("expert", None),
            P(("groups", "expert"), None),
            P(("groups", "expert")),
        ),
        out_specs=P(("groups", "expert"), None),
        check_vma=False,
    )
```

```python
import functools

import jax
import jax.numpy as jnp
from jax import lax
from jax.experimental import pallas as pl
from jax.experimental.pallas import tpu as pltpu
from jax.sharding import PartitionSpec as P


CAP = 6
SUB = 8
EPS = 1e-05
CORES = 2
F32 = jnp.float32
BF16 = jnp.bfloat16


VMEM = pl.BlockSpec(memory_space=pltpu.VMEM)
SMEM = pl.BlockSpec(memory_space=pltpu.SMEM)


def near(value):
    return pltpu.with_memory_space_constraint(value, pltpu.VMEM)


def room(mebibytes):
    return pltpu.CompilerParams(vmem_limit_bytes=mebibytes << 20)


def far(value):
    return pltpu.with_memory_space_constraint(value, pltpu.HBM)


def dot(a, b):
    return jnp.dot(a, b, preferred_element_type=F32)


def packing(width):
    main = width * CAP // SUB
    tail = width - main
    blocks = main // tail
    return main, tail, blocks


def pre_kernel(experts, z_ref, live_ref, ids_ref, tok_ref, gain_ref, router_ref, *outs):
    pieces, table_ref = outs[:-1], outs[-1]
    rows, width = tok_ref.shape
    main, tail, blocks = packing(width)
    lanes = table_ref.shape[1]
    tok = tok_ref[...].astype(F32)
    scale = lax.rsqrt(jnp.mean(tok * tok, axis=-1, keepdims=True) + EPS)
    normed = (tok * scale * gain_ref[...]).astype(BF16)
    normed_f32 = normed.astype(F32)

    row = lax.broadcasted_iota(jnp.int32, (rows, lanes), 0)
    lane = lax.broadcasted_iota(jnp.int32, (rows, lanes), 1)
    first = jnp.zeros((rows, lanes), jnp.int32)
    second = jnp.zeros((rows, lanes), jnp.int32)
    for t in range(rows):
        first = jnp.where(row == t, ids_ref[0, t], first)
        second = jnp.where(row == t, ids_ref[1, t], second)
    alive = row < live_ref[0]
    logits = [
        jnp.sum(normed_f32 * router_ref[e : e + 1, :].astype(F32), axis=-1, keepdims=True)
        for e in range(experts)
    ]
    logit_first = jnp.zeros((rows, lanes), F32)
    logit_second = jnp.zeros((rows, lanes), F32)
    for e in range(experts):
        logit_first = jnp.where(first == e, logits[e], logit_first)
        logit_second = jnp.where(second == e, logits[e], logit_second)
    prob_first = 1.0 / (1.0 + jnp.exp(logit_second - logit_first))
    prob_second = 1.0 / (1.0 + jnp.exp(logit_first - logit_second))

    r = lane % SUB
    k = (lane // SUB) % experts
    j = lane // (SUB * experts)
    expert = k ^ z_ref[0]
    is_first = first == expert
    is_second = second == expert
    member = jnp.logical_and(jnp.logical_or(is_first, is_second), alive).astype(F32)
    slot = jnp.zeros((rows, lanes), F32)
    for t in range(rows - 1):
        slot = slot + jnp.where(row > t, member[t : t + 1, :], 0.0)
    main_slot = jnp.where(r < CAP, r, SUB)
    tail_slot = jnp.where(r < CAP, SUB, (r - CAP) * blocks + j - 1)
    wanted = jnp.where(j == 0, main_slot, tail_slot).astype(F32)
    placed = jnp.where(slot == wanted, member, 0.0)
    gate = jnp.where(is_first, prob_first, prob_second)
    table_ref[...] = placed * gate

    step = experts * SUB
    pick = placed.astype(BF16)
    for i in range(blocks):
        both = jnp.concatenate([pick[:, :step], pick[:, (1 + i) * step : (2 + i) * step]], axis=0)
        data = jnp.concatenate([normed[:, i * tail : (i + 1) * tail], normed[:, main:]], axis=0)
        block = lax.dot_general(both, data, (((0,), (0,)), ((), ())), preferred_element_type=F32).astype(BF16)
        for n, piece in enumerate(pieces):
            piece[:, i * tail : (i + 1) * tail] = block[n * SUB : (n + 1) * SUB, :]


def pre(tokens, norm_gain, router, expert_ids, live_rows, plane):
    rows, width = tokens.shape
    experts = router.shape[1]
    main, _, blocks = packing(width)
    lanes = (1 + blocks) * experts * SUB
    return pl.pallas_call(
        functools.partial(pre_kernel, experts),
        out_shape=[pltpu.VMEM((SUB, main), BF16)] * experts + [pltpu.VMEM((rows, lanes), F32)],
        in_specs=[SMEM, SMEM, SMEM, VMEM, VMEM, VMEM],
        out_specs=[VMEM] * (experts + 1),
        compiler_params=room(8),
        cost_estimate=pl.CostEstimate(flops=20 * 10**9, bytes_accessed=40 * 10**6, transcendentals=0),
        name="pre",
    )(plane.reshape(1), live_rows, far(expert_ids.T), far(tokens), far(norm_gain.reshape(1, width)), far(router.T))


def ffn_kernel(count, *refs):
    pieces = refs[:count]
    wg_ref, wu_ref, wd_ref = refs[count : count + 3]
    outs, x_ref = refs[count + 3 : -1], refs[-1]
    width = wg_ref.shape[0]
    hidden_width = wg_ref.shape[1]
    main, tail, blocks = packing(width)
    at = 0
    for piece in pieces:
        n = piece.shape[0]
        x_ref[at : at + n, :] = piece[...]
        at += n
    total = at
    size = 128 if total % 128 == 0 else total
    row = lax.broadcasted_iota(jnp.int32, (size, size), 0)
    col = lax.broadcasted_iota(jnp.int32, (size, size), 1)
    same = row // SUB == col // SUB
    in_row = lax.broadcasted_iota(jnp.int32, (size, hidden_width), 0) % SUB

    def chunk(base):
        x = x_ref[pl.ds(base, size), :]
        rest = jnp.zeros((size, tail), F32)
        for i in range(blocks):
            take = jnp.logical_and(same, row % SUB == (col % SUB - CAP) * blocks + i)
            take = jnp.logical_and(take, col % SUB >= CAP)
            rest = rest + dot(take.astype(BF16), x[:, i * tail : (i + 1) * tail])
        rest = rest.astype(BF16)
        gate = dot(x, wg_ref[:main, :]) + dot(rest, wg_ref[main:, :])
        up = dot(x, wu_ref[:main, :]) + dot(rest, wu_ref[main:, :])
        hidden = (gate / (1.0 + jnp.exp(-gate)) * up).astype(BF16)
        upper = jnp.where(in_row < CAP, hidden, jnp.zeros_like(hidden))
        for i in range(blocks):
            give = jnp.logical_and(same, col % SUB == (row % SUB - CAP) * blocks + i)
            give = jnp.logical_and(give, row % SUB >= CAP)
            lower = dot(give.astype(BF16), hidden).astype(BF16)
            cols = slice(i * tail, (i + 1) * tail)
            out = (dot(upper, wd_ref[:, cols]) + dot(lower, wd_ref[:, main:])).astype(BF16)
            x_ref[pl.ds(base, size), cols] = out

    if total == size:
        chunk(0)
    else:
        lax.fori_loop(0, total // size, lambda n, c: (chunk(pl.multiple_of(n * size, size)), c)[1], 0)
    at = 0
    for out in outs:
        n = out.shape[0]
        out[...] = x_ref[at : at + n, :]
        at += n


def ffn(pieces, weights, sizes):
    total, main = sum(sizes), pieces[0].shape[1]
    return pl.pallas_call(
        functools.partial(ffn_kernel, len(pieces)),
        out_shape=[pltpu.VMEM((n, main), BF16) for n in sizes],
        in_specs=[VMEM] * (len(pieces) + 3),
        out_specs=[VMEM] * len(sizes),
        scratch_shapes=[pltpu.VMEM((total, main), BF16)],
        compiler_params=room(16),
        name="ffn",
    )(*map(near, pieces), *map(near, weights))


def add_kernel(count, *refs):
    total = refs[0][...].astype(F32)
    for ref in refs[1:count]:
        total = total + ref[...].astype(F32)
    at = 0
    for out in refs[count:]:
        n = out.shape[0]
        out[...] = total[at : at + n, :].astype(BF16)
        at += n


def add(terms, parts):
    rows, main = terms[0].shape
    return pl.pallas_call(
        functools.partial(add_kernel, len(terms)),
        out_shape=[pltpu.VMEM((rows // parts, main), BF16)] * parts,
        in_specs=[VMEM] * len(terms),
        out_specs=[VMEM] * parts,
        compiler_params=room(4),
        name="add",
    )(*map(near, terms))


def combine_kernel(experts, table_ref, tok_ref, *refs):
    pieces, out_ref = refs[:-1], refs[-1]
    own, others = pieces[: 1 - experts], [p[...] for p in pieces[1 - experts :]]
    width = tok_ref.shape[1]
    main, tail, blocks = packing(width)
    step = experts * SUB
    table = table_ref[...]
    high = table.astype(BF16)
    low = (table - high.astype(F32)).astype(BF16)
    first = own[0][...].astype(F32)
    for ref in own[1:]:
        first = first + ref[...].astype(F32)
    arrived = [first.astype(BF16)] + others
    rest = jnp.zeros((tok_ref.shape[0], tail), F32)
    for i in range(blocks):
        cols = slice(i * tail, (i + 1) * tail)
        data = jnp.concatenate([p[:, cols] for p in arrived], axis=0)
        mine, theirs = slice(0, step), slice((1 + i) * step, (2 + i) * step)
        out_ref[:, cols] = (
            tok_ref[:, cols].astype(F32) + dot(high[:, mine], data) + dot(low[:, mine], data)
        ).astype(BF16)
        rest = rest + dot(high[:, theirs], data) + dot(low[:, theirs], data)
    out_ref[:, main:] = (tok_ref[:, main:].astype(F32) + rest).astype(BF16)


def combine(experts, table, tokens, pieces):
    return pl.pallas_call(
        functools.partial(combine_kernel, experts),
        out_shape=jax.ShapeDtypeStruct(tokens.shape, BF16),
        in_specs=[VMEM] * (2 + len(pieces)),
        out_specs=VMEM,
        compiler_params=room(8),
        name="combine",
    )(near(table), near(tokens), *map(near, pieces))


def local(tokens, norm_gain, router, w_gate, w_up, w_down, expert_ids, live_rows):
    devices = lax.axis_size("expert")
    experts = router.shape[1]
    members = devices // experts
    lines = members // CORES

    def swap(value, distance):
        return lax.ppermute(value, "expert", [(i, i ^ distance) for i in range(devices)])

    plane = lax.axis_index("expert") // members
    *outgoing, table = pre(tokens, norm_gain, router, expert_ids, live_rows, plane)
    weights = [w_gate, w_up, w_down]

    here = {}
    for k in range(experts):
        here[0, k, 0] = swap(outgoing[k], k * members) if k else outgoing[0]
    for k in range(experts):
        for y in range(1, lines):
            here[0, k, y] = swap(here[0, k, 0], y * CORES)
    for k in range(experts):
        for y in range(lines):
            here[1, k, y] = swap(here[0, k, y], 1)
    groups = [list(range(experts // 2, experts)), list(range(experts // 2 - 1, -1, -1))]
    order = [(c, k, y) for c in range(CORES) for g in groups for k in g for y in range(lines)]
    results = ffn([here[o] for o in order], weights, [len(g) * lines * SUB for _ in range(CORES) for g in groups])

    half = {}
    for n, group in enumerate(groups):
        keep, give = results[n], results[len(groups) + n]
        parts = add([keep, swap(give, 1)], len(group) * lines)
        for m, k in enumerate(group):
            mine, theirs = parts[m * lines], parts[m * lines + 1 : (m + 1) * lines]
            half[k] = [mine] + [swap(p, (y + 1) * CORES) for y, p in enumerate(theirs)]
    home = list(half[0])
    for k in range(1, experts):
        (total,) = add(half[k], 1)
        home.append(swap(total, k * members))
    return combine(experts, table, tokens, home)


def solution(mesh):
    return jax.shard_map(
        local,
        mesh=mesh,
        in_specs=(
            P(("groups", "expert"), None),
            P(),
            P(),
            P(None, "expert"),
            P(None, "expert"),
            P("expert", None),
            P(("groups", "expert"), None),
            P(("groups", "expert")),
        ),
        out_specs=P(("groups", "expert"), None),
        check_vma=False,
    )
```

```python
import functools

import jax
import jax.numpy as jnp
from jax import lax
from jax.experimental import pallas as pl
from jax.experimental.pallas import tpu as pltpu
from jax.sharding import PartitionSpec as P


CAP = 6
SUB = 8
EPS = 1e-05
CORES = 2
F32 = jnp.float32
BF16 = jnp.bfloat16


VMEM = pl.BlockSpec(memory_space=pltpu.VMEM)
SMEM = pl.BlockSpec(memory_space=pltpu.SMEM)


def near(value):
    return pltpu.with_memory_space_constraint(value, pltpu.VMEM)


def room(mebibytes):
    return pltpu.CompilerParams(vmem_limit_bytes=mebibytes << 20)


def far(value):
    return pltpu.with_memory_space_constraint(value, pltpu.HBM)


def dot(a, b):
    return jnp.dot(a, b, preferred_element_type=F32)


def packing(width):
    main = width * CAP // SUB
    tail = width - main
    blocks = main // tail
    return main, tail, blocks


def pre_kernel(experts, members, ids_ref, tok_ref, gain_ref, router_ref, *outs):
    pieces, table_ref = outs[:-1], outs[-1]
    rows, width = tok_ref.shape
    main, tail, blocks = packing(width)
    lanes = table_ref.shape[1]
    tok = tok_ref[...].astype(F32)
    scale = lax.rsqrt(jnp.mean(tok * tok, axis=-1, keepdims=True) + EPS)
    normed = (tok * scale * gain_ref[...]).astype(BF16)
    normed_f32 = normed.astype(F32)

    row = lax.broadcasted_iota(jnp.int32, (rows, lanes), 0)
    lane = lax.broadcasted_iota(jnp.int32, (rows, lanes), 1)
    first = jnp.zeros((rows, lanes), jnp.int32)
    second = jnp.zeros((rows, lanes), jnp.int32)
    for t in range(rows):
        first = jnp.where(row == t, ids_ref[0, t], first)
        second = jnp.where(row == t, ids_ref[1, t], second)
    logits = [
        jnp.sum(normed_f32 * router_ref[e : e + 1, :].astype(F32), axis=-1, keepdims=True)
        for e in range(experts)
    ]
    logit_first = jnp.zeros((rows, lanes), F32)
    logit_second = jnp.zeros((rows, lanes), F32)
    for e in range(experts):
        logit_first = jnp.where(first == e, logits[e], logit_first)
        logit_second = jnp.where(second == e, logits[e], logit_second)
    prob_first = 1.0 / (1.0 + jnp.exp(logit_second - logit_first))
    prob_second = 1.0 / (1.0 + jnp.exp(logit_first - logit_second))

    r = lane % SUB
    k = (lane // SUB) % experts
    j = lane // (SUB * experts)
    expert = k ^ (lax.axis_index("expert") // members)
    is_first = first == expert
    is_second = second == expert
    member = jnp.logical_or(is_first, is_second).astype(F32)
    slot = jnp.zeros((rows, lanes), F32)
    for t in range(rows - 1):
        slot = slot + jnp.where(row > t, member[t : t + 1, :], 0.0)
    main_slot = jnp.where(r < CAP, r, SUB)
    tail_slot = jnp.where(r < CAP, SUB, (r - CAP) * blocks + j - 1)
    wanted = jnp.where(j == 0, main_slot, tail_slot).astype(F32)
    placed = jnp.where(slot == wanted, member, 0.0)
    gate = jnp.where(is_first, prob_first, prob_second)
    table_ref[...] = placed * gate

    step = experts * SUB
    pick = placed.astype(BF16)
    for i in range(blocks):
        both = jnp.concatenate([pick[:, :step], pick[:, (1 + i) * step : (2 + i) * step]], axis=0)
        data = jnp.concatenate([normed[:, i * tail : (i + 1) * tail], normed[:, main:]], axis=0)
        block = lax.dot_general(both, data, (((0,), (0,)), ((), ())), preferred_element_type=F32).astype(BF16)
        for n, piece in enumerate(pieces):
            piece[:, i * tail : (i + 1) * tail] = block[n * SUB : (n + 1) * SUB, :]


def pre(tokens, norm_gain, router, expert_ids, members):
    rows, width = tokens.shape
    experts = router.shape[1]
    main, _, blocks = packing(width)
    lanes = (1 + blocks) * experts * SUB
    return pl.pallas_call(
        functools.partial(pre_kernel, experts, members),
        out_shape=[pltpu.VMEM((SUB, main), BF16)] * experts + [pltpu.VMEM((rows, lanes), F32)],
        in_specs=[SMEM, VMEM, VMEM, VMEM],
        out_specs=[VMEM] * (experts + 1),
        compiler_params=room(8),
        cost_estimate=pl.CostEstimate(flops=20 * 10**9, bytes_accessed=40 * 10**6, transcendentals=0),
        name="pre",
    )(far(expert_ids.T), far(tokens), far(norm_gain.reshape(1, width)), far(router.T))


def ffn_kernel(count, *refs):
    pieces = refs[:count]
    wg_ref, wu_ref, wd_ref = refs[count : count + 3]
    outs, x_ref = refs[count + 3 : -1], refs[-1]
    width = wg_ref.shape[0]
    hidden_width = wg_ref.shape[1]
    main, tail, blocks = packing(width)
    at = 0
    for piece in pieces:
        n = piece.shape[0]
        x_ref[at : at + n, :] = piece[...]
        at += n
    total = at
    size = 128 if total % 128 == 0 else total
    row = lax.broadcasted_iota(jnp.int32, (size, size), 0)
    col = lax.broadcasted_iota(jnp.int32, (size, size), 1)
    same = row // SUB == col // SUB
    in_row = lax.broadcasted_iota(jnp.int32, (size, hidden_width), 0) % SUB

    def chunk(base):
        x = x_ref[pl.ds(base, size), :]
        rest = jnp.zeros((size, tail), F32)
        for i in range(blocks):
            take = jnp.logical_and(same, row % SUB == (col % SUB - CAP) * blocks + i)
            take = jnp.logical_and(take, col % SUB >= CAP)
            rest = rest + dot(take.astype(BF16), x[:, i * tail : (i + 1) * tail])
        rest = rest.astype(BF16)
        gate = dot(x, wg_ref[:main, :]) + dot(rest, wg_ref[main:, :])
        up = dot(x, wu_ref[:main, :]) + dot(rest, wu_ref[main:, :])
        hidden = (gate / (1.0 + jnp.exp(-gate)) * up).astype(BF16)
        upper = jnp.where(in_row < CAP, hidden, jnp.zeros_like(hidden))
        for i in range(blocks):
            give = jnp.logical_and(same, col % SUB == (row % SUB - CAP) * blocks + i)
            give = jnp.logical_and(give, row % SUB >= CAP)
            lower = dot(give.astype(BF16), hidden).astype(BF16)
            cols = slice(i * tail, (i + 1) * tail)
            out = (dot(upper, wd_ref[:, cols]) + dot(lower, wd_ref[:, main:])).astype(BF16)
            x_ref[pl.ds(base, size), cols] = out

    if total == size:
        chunk(0)
    else:
        lax.fori_loop(0, total // size, lambda n, c: (chunk(pl.multiple_of(n * size, size)), c)[1], 0)
    at = 0
    for out in outs:
        n = out.shape[0]
        out[...] = x_ref[at : at + n, :]
        at += n


def ffn(pieces, weights, sizes):
    total, main = sum(sizes), pieces[0].shape[1]
    return pl.pallas_call(
        functools.partial(ffn_kernel, len(pieces)),
        out_shape=[pltpu.VMEM((n, main), BF16) for n in sizes],
        in_specs=[VMEM] * (len(pieces) + 3),
        out_specs=[VMEM] * len(sizes),
        scratch_shapes=[pltpu.VMEM((total, main), BF16)],
        compiler_params=room(16),
        name="ffn",
    )(*map(near, pieces), *map(near, weights))


def add_kernel(count, *refs):
    total = refs[0][...].astype(F32)
    for ref in refs[1:count]:
        total = total + ref[...].astype(F32)
    at = 0
    for out in refs[count:]:
        n = out.shape[0]
        out[...] = total[at : at + n, :].astype(BF16)
        at += n


def add(terms, parts):
    rows, main = terms[0].shape
    return pl.pallas_call(
        functools.partial(add_kernel, len(terms)),
        out_shape=[pltpu.VMEM((rows // parts, main), BF16)] * parts,
        in_specs=[VMEM] * len(terms),
        out_specs=[VMEM] * parts,
        compiler_params=room(4),
        name="add",
    )(*map(near, terms))


def combine_kernel(experts, live_ref, table_ref, tok_ref, *refs):
    pieces, out_ref = refs[:-1], refs[-1]
    own, others = pieces[: 1 - experts], [p[...] for p in pieces[1 - experts :]]
    width = tok_ref.shape[1]
    main, tail, blocks = packing(width)
    step = experts * SUB
    row = lax.broadcasted_iota(jnp.int32, table_ref.shape, 0)
    table = jnp.where(row < live_ref[0], table_ref[...], 0.0)
    high = table.astype(BF16)
    low = (table - high.astype(F32)).astype(BF16)
    first = own[0][...].astype(F32)
    for ref in own[1:]:
        first = first + ref[...].astype(F32)
    arrived = [first.astype(BF16)] + others
    rest = jnp.zeros((tok_ref.shape[0], tail), F32)
    for i in range(blocks):
        cols = slice(i * tail, (i + 1) * tail)
        data = jnp.concatenate([p[:, cols] for p in arrived], axis=0)
        mine, theirs = slice(0, step), slice((1 + i) * step, (2 + i) * step)
        out_ref[:, cols] = (
            tok_ref[:, cols].astype(F32) + dot(high[:, mine], data) + dot(low[:, mine], data)
        ).astype(BF16)
        rest = rest + dot(high[:, theirs], data) + dot(low[:, theirs], data)
    out_ref[:, main:] = (tok_ref[:, main:].astype(F32) + rest).astype(BF16)


def combine(experts, live_rows, table, tokens, pieces):
    return pl.pallas_call(
        functools.partial(combine_kernel, experts),
        out_shape=jax.ShapeDtypeStruct(tokens.shape, BF16),
        in_specs=[SMEM] + [VMEM] * (2 + len(pieces)),
        out_specs=VMEM,
        compiler_params=room(8),
        name="combine",
    )(live_rows, near(table), near(tokens), *map(near, pieces))


def local(tokens, norm_gain, router, w_gate, w_up, w_down, expert_ids, live_rows):
    devices = lax.axis_size("expert")
    experts = router.shape[1]
    members = devices // experts
    lines = members // CORES

    def swap(value, distance):
        return lax.ppermute(value, "expert", [(i, i ^ distance) for i in range(devices)])

    *outgoing, table = pre(tokens, norm_gain, router, expert_ids, members)
    weights = [w_gate, w_up, w_down]

    here = {}
    for k in range(experts):
        here[0, k, 0] = swap(outgoing[k], k * members) if k else outgoing[0]
    for k in range(experts):
        for y in range(1, lines):
            here[0, k, y] = swap(here[0, k, 0], y * CORES)
    for k in range(experts):
        for y in range(lines):
            here[1, k, y] = swap(here[0, k, y], 1)
    groups = [list(range(experts // 2, experts)), list(range(experts // 2 - 1, -1, -1))]
    order = [(c, k, y) for c in range(CORES) for g in groups for k in g for y in range(lines)]
    results = ffn([here[o] for o in order], weights, [len(g) * lines * SUB for _ in range(CORES) for g in groups])

    half = {}
    for n, group in enumerate(groups):
        keep, give = results[n], results[len(groups) + n]
        parts = add([keep, swap(give, 1)], len(group) * lines)
        for m, k in enumerate(group):
            mine, theirs = parts[m * lines], parts[m * lines + 1 : (m + 1) * lines]
            half[k] = [mine] + [swap(p, (y + 1) * CORES) for y, p in enumerate(theirs)]
    home = list(half[0])
    for k in range(1, experts):
        (total,) = add(half[k], 1)
        home.append(swap(total, k * members))
    return combine(experts, live_rows, table, tokens, home)


def solution(mesh):
    return jax.shard_map(
        local,
        mesh=mesh,
        in_specs=(
            P(("groups", "expert"), None),
            P(),
            P(),
            P(None, "expert"),
            P(None, "expert"),
            P("expert", None),
            P(("groups", "expert"), None),
            P(("groups", "expert")),
        ),
        out_specs=P(("groups", "expert"), None),
        check_vma=False,
    )
```

```python
import functools

import jax
import jax.numpy as jnp
from jax import lax
from jax.experimental import pallas as pl
from jax.experimental.pallas import tpu as pltpu
from jax.sharding import PartitionSpec as P


CAP = 6
SUB = 8
EPS = 1e-05
CORES = 2
F32 = jnp.float32
BF16 = jnp.bfloat16


VMEM = pl.BlockSpec(memory_space=pltpu.VMEM)
SMEM = pl.BlockSpec(memory_space=pltpu.SMEM)


def near(value):
    return pltpu.with_memory_space_constraint(value, pltpu.VMEM)


def room(mebibytes):
    return pltpu.CompilerParams(vmem_limit_bytes=mebibytes << 20)


def far(value):
    return pltpu.with_memory_space_constraint(value, pltpu.HBM)


def dot(a, b):
    return jnp.dot(a, b, preferred_element_type=F32)


def packing(width):
    main = width * CAP // SUB
    tail = width - main
    blocks = main // tail
    return main, tail, blocks


def pre_kernel(experts, members, ids_ref, tok_ref, gain_ref, router_ref, *outs):
    pieces, table_ref = outs[:-1], outs[-1]
    rows, width = tok_ref.shape
    main, tail, blocks = packing(width)
    lanes = table_ref.shape[1]
    tok = tok_ref[...].astype(F32)
    scale = lax.rsqrt(jnp.mean(tok * tok, axis=-1, keepdims=True) + EPS)
    normed = (tok * scale * gain_ref[...]).astype(BF16)
    normed_f32 = normed.astype(F32)

    row = lax.broadcasted_iota(jnp.int32, (rows, lanes), 0)
    lane = lax.broadcasted_iota(jnp.int32, (rows, lanes), 1)
    first = jnp.zeros((rows, lanes), jnp.int32)
    second = jnp.zeros((rows, lanes), jnp.int32)
    for t in range(rows):
        first = jnp.where(row == t, ids_ref[0, t], first)
        second = jnp.where(row == t, ids_ref[1, t], second)
    logits = [
        jnp.sum(normed_f32 * router_ref[e : e + 1, :].astype(F32), axis=-1, keepdims=True)
        for e in range(experts)
    ]
    logit_first = jnp.zeros((rows, lanes), F32)
    logit_second = jnp.zeros((rows, lanes), F32)
    for e in range(experts):
        logit_first = jnp.where(first == e, logits[e], logit_first)
        logit_second = jnp.where(second == e, logits[e], logit_second)
    prob_first = 1.0 / (1.0 + jnp.exp(logit_second - logit_first))
    prob_second = 1.0 / (1.0 + jnp.exp(logit_first - logit_second))

    r = lane % SUB
    k = (lane // SUB) % experts
    j = lane // (SUB * experts)
    expert = k ^ (lax.axis_index("expert") // members)
    is_first = first == expert
    is_second = second == expert
    member = jnp.logical_or(is_first, is_second).astype(F32)
    slot = jnp.zeros((rows, lanes), F32)
    for t in range(rows - 1):
        slot = slot + jnp.where(row > t, member[t : t + 1, :], 0.0)
    main_slot = jnp.where(r < CAP, r, SUB)
    tail_slot = jnp.where(r < CAP, SUB, (SUB - CAP) * (j - 1) + r - CAP)
    wanted = jnp.where(j == 0, main_slot, tail_slot).astype(F32)
    placed = jnp.where(slot == wanted, member, 0.0)
    gate = jnp.where(is_first, prob_first, prob_second)
    table_ref[...] = placed * gate

    step = experts * SUB
    pick = placed.astype(BF16)
    for i in range(blocks):
        both = jnp.concatenate([pick[:, :step], pick[:, (1 + i) * step : (2 + i) * step]], axis=0)
        data = jnp.concatenate([normed[:, i * tail : (i + 1) * tail], normed[:, main:]], axis=0)
        block = lax.dot_general(both, data, (((0,), (0,)), ((), ())), preferred_element_type=F32).astype(BF16)
        for n, piece in enumerate(pieces):
            piece[:, i * tail : (i + 1) * tail] = block[n * SUB : (n + 1) * SUB, :]


def pre(tokens, norm_gain, router, expert_ids, members):
    rows, width = tokens.shape
    experts = router.shape[1]
    main, _, blocks = packing(width)
    lanes = (1 + blocks) * experts * SUB
    return pl.pallas_call(
        functools.partial(pre_kernel, experts, members),
        out_shape=[pltpu.VMEM((SUB, main), BF16)] * experts + [pltpu.VMEM((rows, lanes), F32)],
        in_specs=[SMEM, VMEM, VMEM, VMEM],
        out_specs=[VMEM] * (experts + 1),
        compiler_params=room(8),
        cost_estimate=pl.CostEstimate(flops=20 * 10**9, bytes_accessed=40 * 10**6, transcendentals=0),
        name="pre",
    )(far(expert_ids.T), far(tokens), far(norm_gain.reshape(1, width)), far(router.T))


def ffn_kernel(count, *refs):
    pieces = refs[:count]
    wg_ref, wu_ref, wd_ref = refs[count : count + 3]
    outs, x_ref = refs[count + 3 : -1], refs[-1]
    total, width = x_ref.shape
    main, tail, blocks = packing(width)
    spare = SUB - CAP
    cuts = [slice(i * tail, (i + 1) * tail) for i in range(blocks)]
    at = 0
    for piece in pieces:
        for p in range(0, piece.shape[0], SUB):
            x_ref[at : at + SUB, :main] = piece[p : p + SUB, :]
            for i, cut in enumerate(cuts):
                x_ref[at + spare * i : at + spare * (i + 1), main:] = piece[p + CAP : p + SUB, cut]
            x_ref[at + CAP : at + SUB, main:] = jnp.zeros((spare, tail), BF16)
            at += SUB
    size = 128 if total % 128 == 0 else total

    def chunk(base):
        rows = pl.ds(base, size)
        x = x_ref[rows, :]
        gate = dot(x, wg_ref[...])
        up = dot(x, wu_ref[...])
        hidden = (gate / (1.0 + jnp.exp(-gate)) * up).astype(BF16)
        for cut in cuts + [slice(main, width)]:
            x_ref[rows, cut] = dot(hidden, wd_ref[:, cut]).astype(BF16)

    if total == size:
        chunk(0)
    else:
        lax.fori_loop(0, total // size, lambda n, c: (chunk(pl.multiple_of(n * size, size)), c)[1], 0)
    at = 0
    for out in outs:
        for p in range(0, out.shape[0], SUB):
            out[p : p + SUB, :] = x_ref[at : at + SUB, :main]
            for i, cut in enumerate(cuts):
                out[p + CAP : p + SUB, cut] = x_ref[at + spare * i : at + spare * (i + 1), main:]
            at += SUB


def ffn(pieces, weights, sizes):
    total, main, width = sum(sizes), pieces[0].shape[1], weights[0].shape[0]
    return pl.pallas_call(
        functools.partial(ffn_kernel, len(pieces)),
        out_shape=[pltpu.VMEM((n, main), BF16) for n in sizes],
        in_specs=[VMEM] * (len(pieces) + 3),
        out_specs=[VMEM] * len(sizes),
        scratch_shapes=[pltpu.VMEM((total, width), BF16)],
        compiler_params=room(24),
        name="ffn",
    )(*map(near, pieces), *map(near, weights))


def add_kernel(count, *refs):
    total = refs[0][...].astype(F32)
    for ref in refs[1:count]:
        total = total + ref[...].astype(F32)
    at = 0
    for out in refs[count:]:
        n = out.shape[0]
        out[...] = total[at : at + n, :].astype(BF16)
        at += n


def add(terms, parts):
    rows, main = terms[0].shape
    return pl.pallas_call(
        functools.partial(add_kernel, len(terms)),
        out_shape=[pltpu.VMEM((rows // parts, main), BF16)] * parts,
        in_specs=[VMEM] * len(terms),
        out_specs=[VMEM] * parts,
        compiler_params=room(4),
        name="add",
    )(*map(near, terms))


def combine_kernel(experts, live_ref, table_ref, tok_ref, *refs):
    pieces, out_ref = refs[:-1], refs[-1]
    own, others = pieces[: 1 - experts], [p[...] for p in pieces[1 - experts :]]
    width = tok_ref.shape[1]
    main, tail, blocks = packing(width)
    step = experts * SUB
    row = lax.broadcasted_iota(jnp.int32, table_ref.shape, 0)
    table = jnp.where(row < live_ref[0], table_ref[...], 0.0)
    high = table.astype(BF16)
    low = (table - high.astype(F32)).astype(BF16)
    first = own[0][...].astype(F32)
    for ref in own[1:]:
        first = first + ref[...].astype(F32)
    arrived = [first.astype(BF16)] + others
    rows = tok_ref.shape[0]
    rest = tok_ref[:, main:].astype(F32)
    for i in range(blocks):
        cols = slice(i * tail, (i + 1) * tail)
        data = jnp.concatenate([p[:, cols] for p in arrived], axis=0)
        mine, theirs = slice(0, step), slice((1 + i) * step, (2 + i) * step)
        sums = dot(jnp.concatenate([high[:, mine], low[:, mine], high[:, theirs], low[:, theirs]], axis=0), data)
        parts = [sums[n * rows : (n + 1) * rows, :] for n in range(4)]
        out_ref[:, cols] = (tok_ref[:, cols].astype(F32) + (parts[0] + parts[1])).astype(BF16)
        rest = rest + (parts[2] + parts[3])
    out_ref[:, main:] = rest.astype(BF16)


def combine(experts, live_rows, table, tokens, pieces):
    return pl.pallas_call(
        functools.partial(combine_kernel, experts),
        out_shape=jax.ShapeDtypeStruct(tokens.shape, BF16),
        in_specs=[SMEM] + [VMEM] * (2 + len(pieces)),
        out_specs=VMEM,
        compiler_params=room(8),
        name="combine",
    )(live_rows, near(table), near(tokens), *map(near, pieces))


def local(tokens, norm_gain, router, w_gate, w_up, w_down, expert_ids, live_rows):
    devices = lax.axis_size("expert")
    experts = router.shape[1]
    members = devices // experts
    lines = members // CORES

    def swap(value, distance):
        return lax.ppermute(value, "expert", [(i, i ^ distance) for i in range(devices)])

    *outgoing, table = pre(tokens, norm_gain, router, expert_ids, members)
    weights = [w_gate, w_up, w_down]

    here = {}
    for k in range(experts):
        here[0, k, 0] = swap(outgoing[k], k * members) if k else outgoing[0]
    for k in range(experts):
        for y in range(1, lines):
            here[0, k, y] = swap(here[0, k, 0], y * CORES)
    for k in range(experts):
        for y in range(lines):
            here[1, k, y] = swap(here[0, k, y], 1)
    groups = [list(range(experts // 2, experts)), list(range(experts // 2 - 1, -1, -1))]
    order = [(c, k, y) for c in range(CORES) for g in groups for k in g for y in range(lines)]
    results = ffn([here[o] for o in order], weights, [len(g) * lines * SUB for _ in range(CORES) for g in groups])

    half = {}
    for n, group in enumerate(groups):
        keep, give = results[n], results[len(groups) + n]
        parts = add([keep, swap(give, 1)], len(group) * lines)
        for m, k in enumerate(group):
            mine, theirs = parts[m * lines], parts[m * lines + 1 : (m + 1) * lines]
            half[k] = [mine] + [swap(p, (y + 1) * CORES) for y, p in enumerate(theirs)]
    home = list(half[0])
    for k in range(1, experts):
        (total,) = add(half[k], 1)
        home.append(swap(total, k * members))
    return combine(experts, live_rows, table, tokens, home)


def solution(mesh):
    return jax.shard_map(
        local,
        mesh=mesh,
        in_specs=(
            P(("groups", "expert"), None),
            P(),
            P(),
            P(None, "expert"),
            P(None, "expert"),
            P("expert", None),
            P(("groups", "expert"), None),
            P(("groups", "expert")),
        ),
        out_specs=P(("groups", "expert"), None),
        check_vma=False,
    )
```

```python
import functools

import jax
import jax.numpy as jnp
from jax import lax
from jax.experimental import pallas as pl
from jax.experimental.pallas import tpu as pltpu
from jax.sharding import PartitionSpec as P


CAP = 6
SUB = 8
EPS = 1e-05
CORES = 2
F32 = jnp.float32
BF16 = jnp.bfloat16


VMEM = pl.BlockSpec(memory_space=pltpu.VMEM)
SMEM = pl.BlockSpec(memory_space=pltpu.SMEM)


def near(value):
    return pltpu.with_memory_space_constraint(value, pltpu.VMEM)


def room(mebibytes):
    return pltpu.CompilerParams(vmem_limit_bytes=mebibytes << 20)


def far(value):
    return pltpu.with_memory_space_constraint(value, pltpu.HBM)


def dot(a, b):
    return jnp.dot(a, b, preferred_element_type=F32)


def packing(width):
    main = width * CAP // SUB
    tail = width - main
    blocks = main // tail
    return main, tail, blocks


def pre_kernel(experts, members, ids_ref, tok_ref, gain_ref, router_ref, *outs):
    pieces, table_ref = outs[:-1], outs[-1]
    rows, width = tok_ref.shape
    main, tail, blocks = packing(width)
    lanes = table_ref.shape[1]
    tok = tok_ref[...].astype(F32)
    scale = lax.rsqrt(jnp.mean(tok * tok, axis=-1, keepdims=True) + EPS)
    normed = (tok * scale * gain_ref[...]).astype(BF16)
    normed_f32 = normed.astype(F32)

    row = lax.broadcasted_iota(jnp.int32, (rows, lanes), 0)
    lane = lax.broadcasted_iota(jnp.int32, (rows, lanes), 1)
    first = jnp.zeros((rows, lanes), jnp.int32)
    second = jnp.zeros((rows, lanes), jnp.int32)
    for t in range(rows):
        first = jnp.where(row == t, ids_ref[0, t], first)
        second = jnp.where(row == t, ids_ref[1, t], second)
    logits = [
        jnp.sum(normed_f32 * router_ref[e : e + 1, :].astype(F32), axis=-1, keepdims=True)
        for e in range(experts)
    ]
    logit_first = jnp.zeros((rows, lanes), F32)
    logit_second = jnp.zeros((rows, lanes), F32)
    for e in range(experts):
        logit_first = jnp.where(first == e, logits[e], logit_first)
        logit_second = jnp.where(second == e, logits[e], logit_second)
    prob_first = 1.0 / (1.0 + jnp.exp(logit_second - logit_first))
    prob_second = 1.0 / (1.0 + jnp.exp(logit_first - logit_second))

    r = lane % SUB
    k = (lane // SUB) % experts
    j = lane // (SUB * experts)
    expert = k ^ (lax.axis_index("expert") // members)
    is_first = first == expert
    is_second = second == expert
    member = jnp.logical_or(is_first, is_second).astype(F32)
    slot = jnp.zeros((rows, lanes), F32)
    for t in range(rows - 1):
        slot = slot + jnp.where(row > t, member[t : t + 1, :], 0.0)
    main_slot = jnp.where(r < CAP, r, SUB)
    tail_slot = jnp.where(r < CAP, SUB, (SUB - CAP) * (j - 1) + r - CAP)
    wanted = jnp.where(j == 0, main_slot, tail_slot).astype(F32)
    placed = jnp.where(slot == wanted, member, 0.0)
    gate = jnp.where(is_first, prob_first, prob_second)
    table_ref[...] = placed * gate

    step = experts * SUB
    pick = placed.astype(BF16)
    for i in range(blocks):
        both = jnp.concatenate([pick[:, :step], pick[:, (1 + i) * step : (2 + i) * step]], axis=0)
        data = jnp.concatenate([normed[:, i * tail : (i + 1) * tail], normed[:, main:]], axis=0)
        block = lax.dot_general(both, data, (((0,), (0,)), ((), ())), preferred_element_type=F32).astype(BF16)
        for n, piece in enumerate(pieces):
            piece[:, i * tail : (i + 1) * tail] = block[n * SUB : (n + 1) * SUB, :]


def pre(tokens, norm_gain, router, expert_ids, members):
    rows, width = tokens.shape
    experts = router.shape[1]
    main, _, blocks = packing(width)
    lanes = (1 + blocks) * experts * SUB
    return pl.pallas_call(
        functools.partial(pre_kernel, experts, members),
        out_shape=[pltpu.VMEM((SUB, main), BF16)] * experts + [pltpu.VMEM((rows, lanes), F32)],
        in_specs=[SMEM, VMEM, VMEM, VMEM],
        out_specs=[VMEM] * (experts + 1),
        compiler_params=room(8),
        cost_estimate=pl.CostEstimate(flops=20 * 10**9, bytes_accessed=40 * 10**6, transcendentals=0),
        name="pre",
    )(far(expert_ids.T), far(tokens), far(norm_gain.reshape(1, width)), far(router.T))


def ffn_kernel(count, *refs):
    pieces = refs[:count]
    weights = [refs[n : n + 3] for n in range(count, count + 3 * CORES, 3)]
    outs, x_ref = refs[count + 3 * CORES : -1], refs[-1]
    total, width = x_ref.shape
    main, tail, blocks = packing(width)
    spare = SUB - CAP
    cuts = [slice(i * tail, (i + 1) * tail) for i in range(blocks)]
    at = 0
    for piece in pieces:
        for p in range(0, piece.shape[0], SUB):
            x_ref[at : at + SUB, :main] = piece[p : p + SUB, :]
            for i, cut in enumerate(cuts):
                x_ref[at + spare * i : at + spare * (i + 1), main:] = piece[p + CAP : p + SUB, cut]
            x_ref[at + CAP : at + SUB, main:] = jnp.zeros((spare, tail), BF16)
            at += SUB
    size = 128 if total % 128 == 0 else total

    def chunk(base):
        rows = pl.ds(base, size)
        x = x_ref[rows, :]
        hidden = []
        for wg_ref, wu_ref, _ in weights:
            gate = dot(x, wg_ref[...])
            up = dot(x, wu_ref[...])
            hidden.append((gate / (1.0 + jnp.exp(-gate)) * up).astype(BF16))
        for cut in cuts + [slice(main, width)]:
            result = dot(hidden[0], weights[0][2][:, cut])
            for h, w in zip(hidden[1:], weights[1:]):
                result = result + dot(h, w[2][:, cut])
            x_ref[rows, cut] = result.astype(BF16)

    if total == size:
        chunk(0)
    else:
        lax.fori_loop(0, total // size, lambda n, c: (chunk(pl.multiple_of(n * size, size)), c)[1], 0)
    at = 0
    for out in outs:
        for p in range(0, out.shape[0], SUB):
            out[p : p + SUB, :] = x_ref[at : at + SUB, :main]
            for i, cut in enumerate(cuts):
                out[p + CAP : p + SUB, cut] = x_ref[at + spare * i : at + spare * (i + 1), main:]
            at += SUB


def ffn(pieces, weights, sizes):
    total, main, width = sum(sizes), pieces[0].shape[1], weights[0].shape[0]
    return pl.pallas_call(
        functools.partial(ffn_kernel, len(pieces)),
        out_shape=[pltpu.VMEM((n, main), BF16) for n in sizes],
        in_specs=[VMEM] * (len(pieces) + len(weights)),
        out_specs=[VMEM] * len(sizes),
        scratch_shapes=[pltpu.VMEM((total, width), BF16)],
        compiler_params=room(24),
        name="ffn",
    )(*map(near, pieces), *map(near, weights))


def add_kernel(count, *refs):
    total = refs[0][...].astype(F32)
    for ref in refs[1:count]:
        total = total + ref[...].astype(F32)
    at = 0
    for out in refs[count:]:
        n = out.shape[0]
        out[...] = total[at : at + n, :].astype(BF16)
        at += n


def add(terms, parts):
    rows, main = terms[0].shape
    return pl.pallas_call(
        functools.partial(add_kernel, len(terms)),
        out_shape=[pltpu.VMEM((rows // parts, main), BF16)] * parts,
        in_specs=[VMEM] * len(terms),
        out_specs=[VMEM] * parts,
        compiler_params=room(4),
        name="add",
    )(*map(near, terms))


def combine_kernel(experts, live_ref, table_ref, tok_ref, *refs):
    pieces, out_ref = refs[:-1], refs[-1]
    own, others = pieces[: 1 - experts], [p[...] for p in pieces[1 - experts :]]
    width = tok_ref.shape[1]
    main, tail, blocks = packing(width)
    step = experts * SUB
    row = lax.broadcasted_iota(jnp.int32, table_ref.shape, 0)
    table = jnp.where(row < live_ref[0], table_ref[...], 0.0)
    high = table.astype(BF16)
    low = (table - high.astype(F32)).astype(BF16)
    first = own[0][...].astype(F32)
    for ref in own[1:]:
        first = first + ref[...].astype(F32)
    arrived = [first.astype(BF16)] + others
    rows = tok_ref.shape[0]
    rest = tok_ref[:, main:].astype(F32)
    for i in range(blocks):
        cols = slice(i * tail, (i + 1) * tail)
        data = jnp.concatenate([p[:, cols] for p in arrived], axis=0)
        mine, theirs = slice(0, step), slice((1 + i) * step, (2 + i) * step)
        sums = dot(jnp.concatenate([high[:, mine], low[:, mine], high[:, theirs], low[:, theirs]], axis=0), data)
        parts = [sums[n * rows : (n + 1) * rows, :] for n in range(4)]
        out_ref[:, cols] = (tok_ref[:, cols].astype(F32) + (parts[0] + parts[1])).astype(BF16)
        rest = rest + (parts[2] + parts[3])
    out_ref[:, main:] = rest.astype(BF16)


def combine(experts, live_rows, table, tokens, pieces):
    return pl.pallas_call(
        functools.partial(combine_kernel, experts),
        out_shape=jax.ShapeDtypeStruct(tokens.shape, BF16),
        in_specs=[SMEM] + [VMEM] * (2 + len(pieces)),
        out_specs=VMEM,
        compiler_params=room(8),
        name="combine",
    )(live_rows, near(table), near(tokens), *map(near, pieces))


def local(tokens, norm_gain, router, w_gate, w_up, w_down, expert_ids, live_rows):
    devices = lax.axis_size("expert")
    experts = router.shape[1]
    members = devices // experts
    lines = members // CORES

    def swap(value, distance):
        return lax.ppermute(value, "expert", [(i, i ^ distance) for i in range(devices)])

    *outgoing, table = pre(tokens, norm_gain, router, expert_ids, members)
    weights = [w_gate, w_up, w_down] + [swap(w, 1) for w in (w_gate, w_up, w_down)]

    here = {}
    for k in range(experts):
        here[k, 0] = swap(outgoing[k], k * members) if k else outgoing[0]
    for k in range(experts):
        for y in range(1, lines):
            here[k, y] = swap(here[k, 0], y * CORES)
    order = [(k, y) for k in range(experts) for y in range(lines)]
    results = dict(zip(order, ffn([here[o] for o in order], weights, [SUB] * len(order))))

    half = {}
    for k in range(experts):
        half[k] = [results[k, 0]] + [swap(results[k, y], y * CORES) for y in range(1, lines)]
    home = list(half[0])
    for k in range(1, experts):
        (total,) = add(half[k], 1)
        home.append(swap(total, k * members))
    return combine(experts, live_rows, table, tokens, home)


def solution(mesh):
    return jax.shard_map(
        local,
        mesh=mesh,
        in_specs=(
            P(("groups", "expert"), None),
            P(),
            P(),
            P(None, "expert"),
            P(None, "expert"),
            P("expert", None),
            P(("groups", "expert"), None),
            P(("groups", "expert")),
        ),
        out_specs=P(("groups", "expert"), None),
        check_vma=False,
    )
```

```python
import functools

import jax
import jax.numpy as jnp
from jax import lax
from jax.experimental import pallas as pl
from jax.experimental.pallas import tpu as pltpu
from jax.sharding import PartitionSpec as P


CAP = 6
SUB = 8
EPS = 1e-05
CORES = 2
F32 = jnp.float32
BF16 = jnp.bfloat16


VMEM = pl.BlockSpec(memory_space=pltpu.VMEM)
SMEM = pl.BlockSpec(memory_space=pltpu.SMEM)


def near(value):
    return pltpu.with_memory_space_constraint(value, pltpu.VMEM)


def room(mebibytes):
    return pltpu.CompilerParams(vmem_limit_bytes=mebibytes << 20)


def far(value):
    return pltpu.with_memory_space_constraint(value, pltpu.HBM)


def dot(a, b):
    return jnp.dot(a, b, preferred_element_type=F32)


def packing(width):
    main = width * CAP // SUB
    tail = width - main
    blocks = main // tail
    return main, tail, blocks


def pre_kernel(experts, members, ids_ref, tok_ref, gain_ref, router_ref, *outs):
    pieces, table_ref = outs[:-1], outs[-1]
    rows, width = tok_ref.shape
    main, tail, blocks = packing(width)
    lanes = table_ref.shape[1]
    tok = tok_ref[...].astype(F32)
    scale = lax.rsqrt(jnp.mean(tok * tok, axis=-1, keepdims=True) + EPS)
    normed = (tok * scale * gain_ref[...]).astype(BF16)
    normed_f32 = normed.astype(F32)

    row = lax.broadcasted_iota(jnp.int32, (rows, lanes), 0)
    lane = lax.broadcasted_iota(jnp.int32, (rows, lanes), 1)
    first = jnp.zeros((rows, lanes), jnp.int32)
    second = jnp.zeros((rows, lanes), jnp.int32)
    for t in range(rows):
        first = jnp.where(row == t, ids_ref[0, t], first)
        second = jnp.where(row == t, ids_ref[1, t], second)
    logits = [
        jnp.sum(normed_f32 * router_ref[e : e + 1, :].astype(F32), axis=-1, keepdims=True)
        for e in range(experts)
    ]
    logit_first = jnp.zeros((rows, lanes), F32)
    logit_second = jnp.zeros((rows, lanes), F32)
    for e in range(experts):
        logit_first = jnp.where(first == e, logits[e], logit_first)
        logit_second = jnp.where(second == e, logits[e], logit_second)
    prob_first = 1.0 / (1.0 + jnp.exp(logit_second - logit_first))
    prob_second = 1.0 / (1.0 + jnp.exp(logit_first - logit_second))

    r = lane % SUB
    k = (lane // SUB) % experts
    j = lane // (SUB * experts)
    expert = k ^ (lax.axis_index("expert") // members)
    is_first = first == expert
    is_second = second == expert
    member = jnp.logical_or(is_first, is_second).astype(F32)
    slot = jnp.zeros((rows, lanes), F32)
    for t in range(rows - 1):
        slot = slot + jnp.where(row > t, member[t : t + 1, :], 0.0)
    main_slot = jnp.where(r < CAP, r, SUB)
    tail_slot = jnp.where(r < CAP, SUB, (SUB - CAP) * (j - 1) + r - CAP)
    wanted = jnp.where(j == 0, main_slot, tail_slot).astype(F32)
    placed = jnp.where(slot == wanted, member, 0.0)
    gate = jnp.where(is_first, prob_first, prob_second)
    table_ref[...] = placed * gate

    step = experts * SUB
    pick = placed.astype(BF16)
    for i in range(blocks):
        both = jnp.concatenate([pick[:, :step], pick[:, (1 + i) * step : (2 + i) * step]], axis=0)
        data = jnp.concatenate([normed[:, i * tail : (i + 1) * tail], normed[:, main:]], axis=0)
        block = lax.dot_general(both, data, (((0,), (0,)), ((), ())), preferred_element_type=F32).astype(BF16)
        for n, piece in enumerate(pieces):
            piece[:, i * tail : (i + 1) * tail] = block[n * SUB : (n + 1) * SUB, :]


def pre(tokens, norm_gain, router, expert_ids, members):
    rows, width = tokens.shape
    experts = router.shape[1]
    main, _, blocks = packing(width)
    lanes = (1 + blocks) * experts * SUB
    return pl.pallas_call(
        functools.partial(pre_kernel, experts, members),
        out_shape=[pltpu.VMEM((SUB, main), BF16)] * experts + [pltpu.VMEM((rows, lanes), F32)],
        in_specs=[SMEM, VMEM, VMEM, VMEM],
        out_specs=[VMEM] * (experts + 1),
        compiler_params=room(8),
        cost_estimate=pl.CostEstimate(flops=20 * 10**9, bytes_accessed=40 * 10**6, transcendentals=0),
        name="pre",
    )(far(expert_ids.T), far(tokens), far(norm_gain.reshape(1, width)), far(router.T))


def ffn_kernel(count, *refs):
    pieces = refs[:count]
    weights = [refs[n : n + 3] for n in range(count, count + 3 * CORES, 3)]
    outs, x_ref = refs[count + 3 * CORES : -1], refs[-1]
    total, width = x_ref.shape
    main, tail, blocks = packing(width)
    spare = SUB - CAP
    cuts = [slice(i * tail, (i + 1) * tail) for i in range(blocks)]
    at = 0
    for piece in pieces:
        for p in range(0, piece.shape[0], SUB):
            x_ref[at : at + SUB, :main] = piece[p : p + SUB, :]
            for i, cut in enumerate(cuts):
                x_ref[at + spare * i : at + spare * (i + 1), main:] = piece[p + CAP : p + SUB, cut]
            x_ref[at + CAP : at + SUB, main:] = jnp.zeros((spare, tail), BF16)
            at += SUB
    size = 128 if total % 128 == 0 else total
    direct = total == size

    def chunk(base):
        rows = pl.ds(base, size)
        x = x_ref[rows, :]
        hidden = []
        for wg_ref, wu_ref, _ in weights:
            gate = dot(x, wg_ref[...])
            up = dot(x, wu_ref[...])
            hidden.append((gate / (1.0 + jnp.exp(-gate)) * up).astype(BF16))

        def down(cut):
            result = dot(hidden[0], weights[0][2][:, cut])
            for h, w in zip(hidden[1:], weights[1:]):
                result = result + dot(h, w[2][:, cut])
            return result.astype(BF16)

        rest = down(slice(main, width))
        if direct:
            x_ref[rows, main:] = rest
        for cut in cuts:
            result = down(cut)
            if not direct:
                x_ref[rows, cut] = result
                continue
            for n, out in enumerate(outs):
                out[:, cut] = result[n * SUB : (n + 1) * SUB, :]
        if not direct:
            x_ref[rows, main:] = rest

    if direct:
        chunk(0)
    else:
        lax.fori_loop(0, total // size, lambda n, c: (chunk(pl.multiple_of(n * size, size)), c)[1], 0)
    for n, out in enumerate(outs):
        at = n * SUB
        if not direct:
            out[...] = x_ref[at : at + SUB, :main]
        for i, cut in enumerate(cuts):
            out[CAP:SUB, cut] = x_ref[at + spare * i : at + spare * (i + 1), main:]


def ffn(pieces, weights, sizes):
    total, main, width = sum(sizes), pieces[0].shape[1], weights[0].shape[0]
    return pl.pallas_call(
        functools.partial(ffn_kernel, len(pieces)),
        out_shape=[pltpu.VMEM((n, main), BF16) for n in sizes],
        in_specs=[VMEM] * (len(pieces) + len(weights)),
        out_specs=[VMEM] * len(sizes),
        scratch_shapes=[pltpu.VMEM((total, width), BF16)],
        compiler_params=room(24),
        name="ffn",
    )(*map(near, pieces), *map(near, weights))


def add_kernel(count, *refs):
    total = refs[0][...].astype(F32)
    for ref in refs[1:count]:
        total = total + ref[...].astype(F32)
    at = 0
    for out in refs[count:]:
        n = out.shape[0]
        out[...] = total[at : at + n, :].astype(BF16)
        at += n


def add(terms, parts):
    rows, main = terms[0].shape
    return pl.pallas_call(
        functools.partial(add_kernel, len(terms)),
        out_shape=[pltpu.VMEM((rows // parts, main), BF16)] * parts,
        in_specs=[VMEM] * len(terms),
        out_specs=[VMEM] * parts,
        compiler_params=room(4),
        name="add",
    )(*map(near, terms))


def combine_kernel(experts, live_ref, table_ref, tok_ref, *refs):
    pieces, out_ref = refs[:-1], refs[-1]
    own, others = pieces[: 1 - experts], [p[...] for p in pieces[1 - experts :]]
    width = tok_ref.shape[1]
    main, tail, blocks = packing(width)
    step = experts * SUB
    row = lax.broadcasted_iota(jnp.int32, table_ref.shape, 0)
    table = jnp.where(row < live_ref[0], table_ref[...], 0.0)
    high = table.astype(BF16)
    low = (table - high.astype(F32)).astype(BF16)
    first = own[0][...].astype(F32)
    for ref in own[1:]:
        first = first + ref[...].astype(F32)
    arrived = [first.astype(BF16)] + others
    rows = tok_ref.shape[0]
    rest = tok_ref[:, main:].astype(F32)
    for i in range(blocks):
        cols = slice(i * tail, (i + 1) * tail)
        data = jnp.concatenate([p[:, cols] for p in arrived], axis=0)
        mine, theirs = slice(0, step), slice((1 + i) * step, (2 + i) * step)
        sums = dot(jnp.concatenate([high[:, mine], low[:, mine], high[:, theirs], low[:, theirs]], axis=0), data)
        parts = [sums[n * rows : (n + 1) * rows, :] for n in range(4)]
        out_ref[:, cols] = (tok_ref[:, cols].astype(F32) + (parts[0] + parts[1])).astype(BF16)
        rest = rest + (parts[2] + parts[3])
    out_ref[:, main:] = rest.astype(BF16)


def combine(experts, live_rows, table, tokens, pieces):
    return pl.pallas_call(
        functools.partial(combine_kernel, experts),
        out_shape=jax.ShapeDtypeStruct(tokens.shape, BF16),
        in_specs=[SMEM] + [VMEM] * (2 + len(pieces)),
        out_specs=VMEM,
        compiler_params=room(8),
        name="combine",
    )(live_rows, near(table), near(tokens), *map(near, pieces))


def local(tokens, norm_gain, router, w_gate, w_up, w_down, expert_ids, live_rows):
    devices = lax.axis_size("expert")
    experts = router.shape[1]
    members = devices // experts
    lines = members // CORES

    def swap(value, distance):
        return lax.ppermute(value, "expert", [(i, i ^ distance) for i in range(devices)])

    *outgoing, table = pre(tokens, norm_gain, router, expert_ids, members)
    weights = [w_gate, w_up, w_down] + [swap(w, 1) for w in (w_gate, w_up, w_down)]

    here = {}
    for k in range(experts):
        here[k, 0] = swap(outgoing[k], k * members) if k else outgoing[0]
    for k in range(experts):
        for y in range(1, lines):
            here[k, y] = swap(here[k, 0], y * CORES)
    order = [(k, y) for k in range(experts) for y in range(lines)]
    results = dict(zip(order, ffn([here[o] for o in order], weights, [SUB] * len(order))))

    half = {}
    for k in range(experts):
        half[k] = [results[k, 0]] + [swap(results[k, y], y * CORES) for y in range(1, lines)]
    home = list(half[0])
    for k in range(1, experts):
        (total,) = add(half[k], 1)
        home.append(swap(total, k * members))
    return combine(experts, live_rows, table, tokens, home)


def solution(mesh):
    return jax.shard_map(
        local,
        mesh=mesh,
        in_specs=(
            P(("groups", "expert"), None),
            P(),
            P(),
            P(None, "expert"),
            P(None, "expert"),
            P("expert", None),
            P(("groups", "expert"), None),
            P(("groups", "expert")),
        ),
        out_specs=P(("groups", "expert"), None),
        check_vma=False,
    )
```
